32 devices in a mesh: groups: 2 (over x), replica: 16 (over z, y, core).
Axes of the slice: x: 2, y: 2, z: 4, core: 2. Of those that a mesh axis runs over, the one named last changes fastest.
Arguments:
- tokens: bfloat16 [32768, 2048], P(('groups', 'replica')), parts along dimension 0, may hold values from -6 to 6
- pseudo_keys: bfloat16 [32, 2048, 512], P(('groups', 'replica')), parts along dimension 0, may hold values from -0.875 to 0.875
- pseudo_values: bfloat16 [32, 2048, 512], P(('groups', 'replica')), parts along dimension 0, may hold values from -0.875 to 0.875
- master_keys: float32 [4096, 512], P(('groups', 'replica')), parts along dimension 0, may hold values from -0.125 to 0.125
- moment_keys: float32 [4096, 512], P(('groups', 'replica')), parts along dimension 0, may hold values from -0.125 to 0.125
- master_values: float32 [4096, 512], P(('groups', 'replica')), parts along dimension 0, may hold values from -0.125 to 0.125
- moment_values: float32 [4096, 512], P(('groups', 'replica')), parts along dimension 0, may hold values from -0.125 to 0.125
- outer_hyper: float32 [4], P('groups'), parts along dimension 0, may hold values from 0.5 to 0.95
Outputs:
- eval_keys: bfloat16 [32768, 512], P(('groups', 'replica')), parts along dimension 0
- eval_values: bfloat16 [32768, 512], P(('groups', 'replica')), parts along dimension 0
- new_master_keys: float32 [4096, 512], P(('groups', 'replica')), parts along dimension 0
- new_moment_keys: float32 [4096, 512], P(('groups', 'replica')), parts along dimension 0
- new_master_values: float32 [4096, 512], P(('groups', 'replica')), parts along dimension 0
- new_moment_values: float32 [4096, 512], P(('groups', 'replica')), parts along dimension 0
The draws below stay inside these ranges and needn't reach their ends.
There are 2 independent parts, one for each index of `groups`. The reference program is written for one: setup_inputs(seed, part) draws one part's arguments, and reference() takes and returns one part's arrays. A program takes and returns all parts, laid end to end along the dimension named above; each array names one. Nothing has to cross between parts.
All inputs are finite; a program needn't handle non-finite values.
Results may differ from the reference program's by a relative error of at most 0.0049.
Values may be sent and summed in bfloat16 or wider, within the bound.
No kernel may reach another device: no remote copies, remote signals or barrier semaphores. Data moves between devices by JAX's collectives and lax.ppermute only.
A program may use at most 128 MiB of HBM per device.

```python
import jax
import jax.numpy as jnp

D = 2048
KVW = 512
TOKENS = 16384
N_REPLICA = 16


def with_spikes(array, stream_key, source, target, blocks, factor):
    owner, partner = [(jnp.arange(array.shape[position]) // (array.shape[position] // blocks)).reshape([-1 if axis == position else 1 for axis in range(array.ndim)]) for position in (source, target)]
    chosen = jax.random.permutation(stream_key, blocks)[partner]
    strong = (owner == chosen) | (owner == (partner + blocks // 2) % blocks)
    return jnp.where(strong, factor * array, array)


def levels(rng, shape, pieces, least, high):
    def one(dim, shards_of):
        heights = jax.random.uniform(jax.random.fold_in(jax.random.fold_in(rng, 6), dim), (shards_of,), jnp.float32, least / len(pieces), high / len(pieces))
        return jnp.repeat(jnp.exp(heights), shape[dim] // shards_of).reshape((-1,) + (1,) * (len(shape) - dim - 1))

    loudness = one(*pieces[0])
    for cut in pieces[1:]:
        loudness = loudness * one(*cut)
    return loudness


def gaussian(rng, dims, spread, limit, pieces=(), held_as=jnp.bfloat16):
    values = spread * jax.random.normal(rng, dims, jnp.float32)
    if pieces:
        values = values * levels(rng, dims, pieces, -0.22, 0.18)
    return jnp.clip(values, -limit, limit).astype(held_as)


def bell_draw_with(stream_key, dims, deviation, limit, pieces, heavy, dtype=jnp.bfloat16):
    drawn = deviation * jax.random.normal(stream_key, dims, jnp.float32)
    if pieces:
        drawn = drawn * levels(stream_key, dims, pieces, -0.22, 0.18)
    return jnp.clip(with_spikes(drawn, jax.random.fold_in(stream_key, 3), *heavy), -limit, limit).astype(dtype)


def setup_inputs(seed: int = 0, part: int = 0) -> dict:
    arg_keys = jax.random.split(jax.random.key(seed), 9)
    part_keys = jax.random.split(jax.random.fold_in(arg_keys[8], part), 9)
    return {
        "tokens": gaussian(part_keys[0], (TOKENS, D), 1.0, 6.0, ((0, 16),)),
        "pseudo_keys": bell_draw_with(part_keys[1], (N_REPLICA, D, KVW), 0.1, 0.875, ((0, 16),), (0, 1, 16, 2.0)),
        "pseudo_values": bell_draw_with(part_keys[2], (N_REPLICA, D, KVW), 0.1, 0.875, ((0, 16),), (0, 1, 16, 2.0)),
        "master_keys": gaussian(part_keys[3], (D, KVW), D ** -0.5, 0.125, ((0, 16),), jnp.float32),
        "moment_keys": gaussian(part_keys[4], (D, KVW), 0.02, 0.125, ((0, 16),), jnp.float32),
        "master_values": gaussian(part_keys[5], (D, KVW), D ** -0.5, 0.125, ((0, 16),), jnp.float32),
        "moment_values": gaussian(part_keys[6], (D, KVW), 0.02, 0.125, ((0, 16),), jnp.float32),
        "outer_hyper": jnp.clip(jax.random.uniform(part_keys[7], (2,), jnp.float32, 0.5, 0.95), 0.5, 0.95),
    }


def outer_update(pseudo, master, moment, outer_rate, outer_mom):
    averaged = jnp.sum(pseudo.astype(jnp.float32), axis=0) / N_REPLICA
    moment_new = outer_mom * moment + averaged
    master_new = master - outer_rate * (averaged + outer_mom * moment_new)
    return master_new, moment_new


def reference(tokens, pseudo_keys, pseudo_values, master_keys, moment_keys, master_values, moment_values, outer_hyper):
    outer_rate = outer_hyper[0]
    outer_mom = outer_hyper[1]
    master_k, moment_k = outer_update(pseudo_keys, master_keys, moment_keys, outer_rate, outer_mom)
    master_v, moment_v = outer_update(pseudo_values, master_values, moment_values, outer_rate, outer_mom)
    eval_keys = jnp.dot(tokens, master_k.astype(jnp.bfloat16), preferred_element_type=jnp.float32).astype(jnp.bfloat16)
    eval_values = jnp.dot(tokens, master_v.astype(jnp.bfloat16), preferred_element_type=jnp.float32).astype(jnp.bfloat16)
    return (eval_keys, eval_values, master_k, moment_k, master_v, moment_v)
```

```python
import jax
import jax.numpy as jnp
from jax import lax
from jax.sharding import PartitionSpec as P


def swap(array, stride):
    replicas = lax.axis_size("replica")
    return lax.ppermute(array, "replica", [(r, r ^ stride) for r in range(replicas)])


def pick(array, start, count):
    return lax.dynamic_slice_in_dim(array, start, count, 0)


def wide(array):
    return array.astype(jnp.float32)


def body(
    tokens,
    pseudo_keys,
    pseudo_values,
    master_keys,
    moment_keys,
    master_values,
    moment_values,
    outer_hyper,
):
    outer_rate = outer_hyper[0]
    outer_mom = outer_hyper[1]
    replicas = lax.axis_size("replica")
    rows, width = master_keys.shape
    depth = replicas // 4
    half = depth // 2
    me = lax.axis_index("replica")
    core, y, z = me % 2, (me // 2) % 2, me // 4
    near_at = (z // half) * half
    far_at = half - near_at

    def reduce_core(pseudo):
        blocks = pseudo[0].reshape(depth, 2, 2, rows, width)

        def part(row, side):
            piece = lax.dynamic_slice(blocks, (0, row, side, 0, 0), (depth, 1, 1, rows, width))
            return piece.reshape(depth, rows, width)

        other_in = swap(part(1 - y, 1 - core), 1)
        mine_in = swap(part(y, 1 - core), 1)
        other = (wide(part(1 - y, core)) + wide(other_in)).astype(jnp.bfloat16)
        return other, (part(y, core), mine_in)

    def reduce_y(other, mine):
        def add(at):
            arrived = swap(pick(other, at, half), 2)
            return wide(pick(mine[0], at, half)) + wide(pick(mine[1], at, half)) + wide(arrived)

        return add(far_at), add(near_at)

    def reduce_z(far, near):
        def row(j):
            block = far if j >= half else near
            return pick(block, (z ^ j) % half, 1)[0]

        order = list(range(half, depth)) + list(range(1, half))
        arrived = [swap(row(j).astype(jnp.bfloat16), 4 * j) for j in order]
        total = row(0)
        for piece in arrived:
            total = total + wide(piece)
        return total

    def nesterov(summed, master, moment):
        averaged = summed / replicas
        moment_new = outer_mom * moment + averaged
        master_new = master - outer_rate * (averaged + outer_mom * moment_new)
        return (master_new, moment_new)

    def gather(weights):
        slabs = [weights] + [swap(weights, 4 * j) for j in range(1, depth)]
        whole = jnp.zeros((depth, 2, 2, rows, width), jnp.bfloat16)
        for first in (0, half):
            group = jnp.stack(slabs[first : first + half])
            pair = jnp.stack([group, swap(group, 2)])
            quad = jnp.stack([pair, swap(pair, 1)])
            for j in range(half):
                for side in range(2):
                    for row in range(2):
                        at = (z ^ (first + j), y ^ row, core ^ side, 0, 0)
                        piece = quad[side, row, j].reshape(1, 1, 1, rows, width)
                        whole = lax.dynamic_update_slice(whole, piece, at)
        return whole.reshape(replicas * rows, width)

    other_k, mine_k = reduce_core(pseudo_keys)
    other_v, mine_v = reduce_core(pseudo_values)
    far_k, near_k = reduce_y(other_k, mine_k)
    far_v, near_v = reduce_y(other_v, mine_v)
    summed_keys = reduce_z(far_k, near_k)
    summed_values = reduce_z(far_v, near_v)
    master_k, moment_k = nesterov(summed_keys, master_keys, moment_keys)
    master_v, moment_v = nesterov(summed_values, master_values, moment_values)
    whole_keys = gather(master_k.astype(jnp.bfloat16))
    whole_values = gather(master_v.astype(jnp.bfloat16))
    projected_keys = jnp.dot(tokens, whole_keys, preferred_element_type=jnp.float32)
    projected_values = jnp.dot(tokens, whole_values, preferred_element_type=jnp.float32)
    return (
        projected_keys.astype(jnp.bfloat16),
        projected_values.astype(jnp.bfloat16),
        master_k,
        moment_k,
        master_v,
        moment_v,
    )


def solution(mesh):
    spec = P(("groups", "replica"), None)
    stacked = P(("groups", "replica"), None, None)
    in_specs = (spec, stacked, stacked, spec, spec, spec, spec, P("groups"))
    out_specs = (spec,) * 6
    return jax.shard_map(body, mesh=mesh, in_specs=in_specs, out_specs=out_specs, check_vma=False)
```

```python
import functools

import jax
import jax.numpy as jnp
from jax import lax
from jax.experimental import pallas as pl
from jax.experimental.pallas import tpu as pltpu
from jax.sharding import PartitionSpec as P


BF16, F32 = jnp.bfloat16, jnp.float32
IN_VMEM = pl.BlockSpec(memory_space=pltpu.VMEM)
IN_HBM = pl.BlockSpec(memory_space=pltpu.HBM)


def swap(array, stride):
    replicas = lax.axis_size("replica")
    return lax.ppermute(array, "replica", [(r, r ^ stride) for r in range(replicas)])


def call(kernel, arrays, out, *, specs=None, scratch=(), hold=True, flops=10**6, **options):
    if specs is None:
        specs = [IN_VMEM] * len(arrays)
    holders = {id(IN_VMEM): pltpu.VMEM, id(IN_HBM): pltpu.HBM}
    arrays = [
        pltpu.with_memory_space_constraint(a, holders[id(spec)]) if id(spec) in holders else a
        for a, spec in zip(arrays, specs)
    ]
    shape = pltpu.VMEM if hold else jax.ShapeDtypeStruct
    return pl.pallas_call(
        kernel,
        out_shape=[shape(*o) for o in out],
        in_specs=specs,
        out_specs=[IN_VMEM] * len(out),
        scratch_shapes=scratch,
        cost_estimate=pl.CostEstimate(flops=flops, bytes_accessed=10**6, transcendentals=0),
        compiler_params=pltpu.CompilerParams(vmem_limit_bytes=8 * 2**20),
        **options,
    )(*arrays)


def copy_kernel(plan, blocks, *refs):
    *outs, sem = refs
    me = lax.axis_index("replica")
    copies = [
        pltpu.make_async_copy(blocks.at[me ^ block], outs[o].at[place], sem.at[n])
        for n, (block, o, place) in enumerate(plan)
    ]
    for copy in copies:
        copy.start()
    for copy in copies:
        copy.wait()


def add_kernel(terms, outs, *refs):
    for o, rows in enumerate(terms):
        out = refs[outs + o]
        for place, parts in enumerate(rows):
            total = None
            for ref, at in parts:
                part = refs[ref][at].astype(F32)
                total = part if total is None else total + part
            out[place] = total.astype(out.dtype)


def nesterov(summed, master, moment, hyper, replicas):
    outer_rate, outer_mom = hyper[:, 0:1], hyper[:, 1:2]
    averaged = summed / replicas
    moment_new = outer_mom * moment + averaged
    master_new = master - outer_rate * (averaged + outer_mom * moment_new)
    return master_new, moment_new


def weights_kernel(replicas, places, hyper, master, moment, *refs):
    *parts, weights, summed = refs
    total = parts[0][places[0]].astype(F32)
    for part, at in zip(parts[1:], places[1:]):
        total = total + part[at].astype(F32)
    summed[...] = total
    master_new, _ = nesterov(total, master[...], moment[...], hyper, replicas)
    weights[0] = master_new.astype(BF16)


def state_kernel(replicas, hyper, master, moment, summed, master_out, moment_out):
    master_new, moment_new = nesterov(
        summed[...], master[...], moment[...], hyper, replicas
    )
    master_out[...] = master_new
    moment_out[...] = moment_new


def product_kernel(height, blocks, groups, tokens, *refs):
    slabs, out = refs[:groups], refs[-1]
    weights = jnp.concatenate([s[...].reshape(-1, s.shape[-1]) for s in slabs], axis=0)
    rows = jnp.concatenate([tokens[:, k * height : (k + 1) * height] for k in blocks], axis=1)
    total = jnp.dot(rows, weights, preferred_element_type=F32)
    if len(refs) > groups + 1:
        total = total + refs[groups][...]
    out[...] = total.astype(out.dtype)


def columns_kernel(rows, tokens, out, sem):
    me = lax.axis_index("replica")
    copies = [
        pltpu.make_async_copy(
            tokens.at[:, pl.ds(pl.multiple_of((me ^ block) * rows, rows), rows)],
            out.at[:, pl.ds(block * rows, rows)],
            sem.at[block],
        )
        for block in range(tokens.shape[1] // rows)
    ]
    for copy in copies:
        copy.start()
    for copy in copies:
        copy.wait()


SUMS = {
    "k": [(4, [4, 6, 12, 14]), (2, [2, 10]), (8, [8])],
    "v": [(2, [2]), (2, [10, 14]), (2, [6]), (4, [4]), (4, [12]), (8, [8])],
}
GATHERS = {
    "k": [(2, [2]), (4, [4]), (8, [8]), (4, [6, 12]), (2, [10]), (4, [14])],
    "v": [(4, [4]), (2, [2]), (8, [8]), (2, [6, 10]), (4, [12]), (2, [14])],
}


def plain_sums(depth):
    half = depth // 2
    far = [4 * j for j in range(half, depth)]
    near = [4 * j for j in range(half)]
    over = [(2, [b + 2 for b in part]) for part in (far, near)]
    return over + [(b, [b]) for b in far + near[1:]]


def plain_gathers(depth):
    return [(stride, blocks) for stride, blocks in reversed(plain_sums(depth))]


def steps_of(groups):
    steps, step, count = [], [], 0
    for n, (blocks, _) in enumerate(groups[:-1]):
        step += [(n, 0), (n, 1)]
        count += 2 * len(blocks)
        if count >= 4:
            steps.append(step)
            step, count = [], 0
    last = len(groups) - 1
    return steps + ([step] if step else []) + [[(last, 0)], [(last, 1)]]


def body(
    tokens,
    pseudo_keys,
    pseudo_values,
    master_keys,
    moment_keys,
    master_values,
    moment_values,
    outer_hyper,
):
    replicas = lax.axis_size("replica")
    rows, width = master_keys.shape
    depth = replicas // 4
    me = lax.axis_index("replica")
    slab = (rows, width)
    hyper = outer_hyper.reshape(1, -1)

    def add(rows_of, dtype):
        arrays = []
        for array, _ in [term for row in rows_of for term in row]:
            if not any(array is other for other in arrays):
                arrays.append(array)
        index = {id(array): n for n, array in enumerate(arrays)}
        terms = [[[(index[id(array)], at) for array, at in row] for row in rows_of]]
        (total,) = call(
            functools.partial(add_kernel, terms, len(arrays)),
            arrays,
            [((len(rows_of), *slab), dtype)],
        )
        return total

    def pieces(pseudo, blocks):
        plan = [(b + side, o, n) for o, side in enumerate((1, 0)) for n, b in enumerate(blocks)]
        return call(
            functools.partial(copy_kernel, plan),
            [pseudo[0].reshape(replicas, *slab)],
            [((len(blocks), *slab), BF16)] * 2,
            specs=[IN_HBM],
            scratch=[pltpu.SemaphoreType.DMA((len(plan),))],
        )

    def reduce(pseudo, transfers):
        order = [b for _, blocks in transfers for b in blocks] + [0]
        terms = {}
        for part in (order[:depth], order[depth:]):
            partner, own = pieces(pseudo, part)
            partner = swap(partner, 1)
            terms.update({b: [(own, n), (partner, n)] for n, b in enumerate(part)})
        for stride, blocks in transfers:
            sent = add([terms[b] for b in blocks], BF16)
            got = swap(sent, stride)
            for n, b in enumerate(blocks):
                terms[b ^ stride].append((got, n))
        return terms[0]

    def weigh(terms, master, moment):
        weights, summed = call(
            functools.partial(weights_kernel, replicas, [at for _, at in terms]),
            [hyper, master, moment, *[array for array, _ in terms]],
            [((1, *slab), BF16), (slab, F32)],
        )
        state = call(
            functools.partial(state_kernel, replicas),
            [hyper, master, moment, summed],
            [(slab, F32)] * 2,
            hold=False,
        )
        return weights, state

    def gather(weights, transfers):
        groups = [([0], weights)]
        for stride, blocks in transfers:
            parents = [b ^ stride for b in blocks]
            held = [array for group, array in groups if group == parents]
            if not held:
                rows_of = [
                    [(array, group.index(b))]
                    for b in parents
                    for group, array in groups
                    if b in group
                ]
                held = [add(rows_of, BF16)]
            groups.append((list(blocks), swap(held[0], stride)))
        pairs = [swap(array, 1) for _, array in groups]
        return groups, pairs

    if rows % 128 == 0:
        (columns,) = call(
            functools.partial(columns_kernel, rows),
            [tokens],
            [(tokens.shape, BF16)],
            specs=[IN_HBM],
            scratch=[pltpu.SemaphoreType.DMA((replicas,))],
        )

    def project(groups, pairs):
        arrivals = [
            [(blocks, array), ([b + 1 for b in blocks], pair)]
            for (blocks, array), pair in zip(groups, pairs)
        ]
        if rows % 128:
            whole = jnp.zeros((replicas, *slab), BF16)
            for blocks, array in [a for both in arrivals for a in both]:
                whole = whole.at[me ^ jnp.array(blocks)].set(array)
            return jnp.dot(tokens, whole.reshape(-1, width), preferred_element_type=F32).astype(BF16)
        total = None
        steps = steps_of(groups)
        for i, step in enumerate(steps):
            last = i == len(steps) - 1
            taken = [arrivals[n][side] for n, side in step]
            blocks = [b for part, _ in taken for b in part]
            arrays = [columns] + [array for _, array in taken] + ([] if total is None else [total])
            (total,) = call(
                functools.partial(product_kernel, rows, blocks, len(step)),
                arrays,
                [((tokens.shape[0], width), BF16 if last else F32)],
                flops=2 * tokens.shape[0] * len(blocks) * rows * width,
                hold=not last,
            )
        return total

    def stream(pseudo, master, moment, s):
        sums = SUMS[s] if depth == 4 else plain_sums(depth)
        gathers = GATHERS[s] if depth == 4 else plain_gathers(depth)
        weights, state = weigh(reduce(pseudo, sums), master, moment)
        return project(*gather(weights, gathers)), state

    projected_keys, state_k = stream(pseudo_keys, master_keys, moment_keys, "k")
    projected_values, state_v = stream(pseudo_values, master_values, moment_values, "v")
    return (projected_keys, projected_values, *state_k, *state_v)


def solution(mesh):
    spec = P(("groups", "replica"), None)
    stacked = P(("groups", "replica"), None, None)
    in_specs = (spec, stacked, stacked, spec, spec, spec, spec, P("groups"))
    out_specs = (spec,) * 6

    return jax.shard_map(body, mesh=mesh, in_specs=in_specs, out_specs=out_specs, check_vma=False)
```

```python
import functools

import jax
import jax.numpy as jnp
from jax import lax
from jax.experimental import pallas as pl
from jax.experimental.pallas import tpu as pltpu
from jax.sharding import PartitionSpec as P


BF16, F32 = jnp.bfloat16, jnp.float32
IN_VMEM = pl.BlockSpec(memory_space=pltpu.VMEM)
IN_HBM = pl.BlockSpec(memory_space=pltpu.HBM)


def swap(array, stride):
    replicas = lax.axis_size("replica")
    return lax.ppermute(array, "replica", [(r, r ^ stride) for r in range(replicas)])


def call(kernel, arrays, out, *, specs=None, scratch=(), hold=True, flops=10**6, **options):
    if specs is None:
        specs = [IN_VMEM] * len(arrays)
    holders = {id(IN_VMEM): pltpu.VMEM, id(IN_HBM): pltpu.HBM}
    arrays = [
        pltpu.with_memory_space_constraint(a, holders[id(spec)]) if id(spec) in holders else a
        for a, spec in zip(arrays, specs)
    ]
    shape = pltpu.VMEM if hold else jax.ShapeDtypeStruct
    return pl.pallas_call(
        kernel,
        out_shape=[shape(*o) for o in out],
        in_specs=specs,
        out_specs=[IN_VMEM] * len(out),
        scratch_shapes=scratch,
        cost_estimate=pl.CostEstimate(flops=flops, bytes_accessed=10**6, transcendentals=0),
        compiler_params=pltpu.CompilerParams(vmem_limit_bytes=12 * 2**20),
        **options,
    )(*arrays)


def copy_kernel(plan, blocks, *refs):
    *outs, sem = refs
    me = lax.axis_index("replica")
    copies = [
        pltpu.make_async_copy(blocks.at[me ^ block], outs[o].at[place], sem.at[n])
        for n, (block, o, place) in enumerate(plan)
    ]
    for copy in copies:
        copy.start()
    for copy in copies:
        copy.wait()


def add_kernel(terms, outs, *refs):
    for o, rows in enumerate(terms):
        out = refs[outs + o]
        for place, parts in enumerate(rows):
            total = None
            for ref, at in parts:
                part = refs[ref][at].astype(F32)
                total = part if total is None else total + part
            out[place] = total.astype(out.dtype)


def nesterov(summed, master, moment, hyper, replicas):
    outer_rate, outer_mom = hyper[:, 0:1], hyper[:, 1:2]
    averaged = summed / replicas
    moment_new = outer_mom * moment + averaged
    master_new = master - outer_rate * (averaged + outer_mom * moment_new)
    return master_new, moment_new


def weights_kernel(replicas, places, hyper, master, moment, *refs):
    *parts, weights, summed = refs
    total = parts[0][places[0]].astype(F32)
    for part, at in zip(parts[1:], places[1:]):
        total = total + part[at].astype(F32)
    summed[...] = total
    master_new, _ = nesterov(total, master[...], moment[...], hyper, replicas)
    weights[0] = master_new.astype(BF16)


def state_kernel(replicas, hyper, master, moment, summed, master_out, moment_out):
    master_new, moment_new = nesterov(
        summed[...], master[...], moment[...], hyper, replicas
    )
    master_out[...] = master_new
    moment_out[...] = moment_new


def product(height, blocks, tokens, slabs):
    weights = jnp.concatenate([s[...].reshape(-1, s.shape[-1]) for s in slabs], axis=0)
    rows = jnp.concatenate([tokens[:, k * height : (k + 1) * height] for k in blocks], axis=1)
    return jnp.dot(rows, weights, preferred_element_type=F32)


def product_kernel(height, blocks, groups, tokens, *refs):
    slabs, out = refs[:groups], refs[-1]
    total = product(height, blocks, tokens, slabs)
    if len(refs) > groups + 1:
        total = total + refs[groups][...]
    out[...] = total


def finish_kernel(height, plans, tokens, *refs):
    refs, outs = refs[: -len(plans)], refs[-len(plans) :]
    step = len(refs) // len(plans)
    for n, (blocks, out) in enumerate(zip(plans, outs)):
        total, *slabs = refs[n * step : (n + 1) * step]
        out[...] = (total[...] + product(height, blocks, tokens, slabs)).astype(out.dtype)


def columns_kernel(rows, tokens, out, sem):
    me = lax.axis_index("replica")
    copies = [
        pltpu.make_async_copy(
            tokens.at[:, pl.ds(pl.multiple_of((me ^ block) * rows, rows), rows)],
            out.at[:, pl.ds(block * rows, rows)],
            sem.at[block],
        )
        for block in range(tokens.shape[1] // rows)
    ]
    for copy in copies:
        copy.start()
    for copy in copies:
        copy.wait()


SUMS = {
    "k": [(4, [12, 14]), (2, [2, 6]), (2, [10]), (4, [4]), (8, [8])],
    "v": [(2, [2]), (2, [10]), (2, [6, 14]), (4, [4]), (4, [12]), (8, [8])],
}
GATHERS = {
    "k": [(4, [4]), (8, [8]), (2, [2]), (4, [6, 12]), (2, [10]), (4, [14])],
    "v": [(4, [4]), (2, [2]), (8, [8]), (4, [12]), (2, [6]), (2, [10]), (2, [14])],
}


def plain_sums(depth):
    half = depth // 2
    far = [4 * j for j in range(half, depth)]
    near = [4 * j for j in range(half)]
    over = [(2, [b + 2 for b in part]) for part in (far, near)]
    return over + [(b, [b]) for b in far + near[1:]]


def plain_gathers(depth):
    return [(stride, blocks) for stride, blocks in reversed(plain_sums(depth))]


def steps_of(groups):
    steps, step, count = [], [], 0
    for n, (blocks, _) in enumerate(groups[:-1]):
        step += [(n, 0), (n, 1)]
        count += 2 * len(blocks)
        if count >= 4:
            steps.append(step)
            step, count = [], 0
    return steps + ([step] if step else [])


def body(
    tokens,
    pseudo_keys,
    pseudo_values,
    master_keys,
    moment_keys,
    master_values,
    moment_values,
    outer_hyper,
):
    replicas = lax.axis_size("replica")
    rows, width = master_keys.shape
    depth = replicas // 4
    me = lax.axis_index("replica")
    slab = (rows, width)
    hyper = outer_hyper.reshape(1, -1)

    def add(rows_of, dtype):
        arrays = []
        for array, _ in [term for row in rows_of for term in row]:
            if not any(array is other for other in arrays):
                arrays.append(array)
        index = {id(array): n for n, array in enumerate(arrays)}
        terms = [[[(index[id(array)], at) for array, at in row] for row in rows_of]]
        (total,) = call(
            functools.partial(add_kernel, terms, len(arrays)),
            arrays,
            [((len(rows_of), *slab), dtype)],
        )
        return total

    def pieces(pseudo, blocks):
        plan = [(b + side, o, n) for o, side in enumerate((1, 0)) for n, b in enumerate(blocks)]
        return call(
            functools.partial(copy_kernel, plan),
            [pseudo[0].reshape(replicas, *slab)],
            [((len(blocks), *slab), BF16)] * 2,
            specs=[IN_HBM],
            scratch=[pltpu.SemaphoreType.DMA((len(plan),))],
        )

    def reduce(pseudo, transfers):
        order = [b for _, blocks in transfers for b in blocks] + [0]
        terms = {}
        for part in (order[:depth], order[depth:]):
            partner, own = pieces(pseudo, part)
            partner = swap(partner, 1)
            terms.update({b: [(own, n), (partner, n)] for n, b in enumerate(part)})
        for stride, blocks in transfers:
            sent = add([terms[b] for b in blocks], BF16)
            got = swap(sent, stride)
            for n, b in enumerate(blocks):
                terms[b ^ stride].append((got, n))
        return terms[0]

    def weigh(terms, master, moment):
        weights, summed = call(
            functools.partial(weights_kernel, replicas, [at for _, at in terms]),
            [hyper, master, moment, *[array for array, _ in terms]],
            [((1, *slab), BF16), (slab, F32)],
        )
        state = call(
            functools.partial(state_kernel, replicas),
            [hyper, master, moment, summed],
            [(slab, F32)] * 2,
            hold=False,
        )
        return weights, state

    def gather(weights, transfers):
        groups = [([0], weights)]
        for stride, blocks in transfers:
            parents = [b ^ stride for b in blocks]
            held = [array for group, array in groups if group == parents]
            if not held:
                rows_of = [
                    [(array, group.index(b))]
                    for b in parents
                    for group, array in groups
                    if b in group
                ]
                held = [add(rows_of, BF16)]
            groups.append((list(blocks), swap(held[0], stride)))
        pairs = [swap(array, 1) for _, array in groups]
        return groups, pairs

    if rows % 128 == 0:
        (columns,) = call(
            functools.partial(columns_kernel, rows),
            [tokens],
            [(tokens.shape, BF16)],
            specs=[IN_HBM],
            scratch=[pltpu.SemaphoreType.DMA((replicas,))],
        )

    def project(groups, pairs):
        arrivals = [
            [(blocks, array), ([b + 1 for b in blocks], pair)]
            for (blocks, array), pair in zip(groups, pairs)
        ]
        if rows % 128:
            whole = jnp.zeros((replicas, *slab), BF16)
            for blocks, array in [a for both in arrivals for a in both]:
                whole = whole.at[me ^ jnp.array(blocks)].set(array)
            return jnp.dot(tokens, whole.reshape(-1, width), preferred_element_type=F32).astype(BF16)
        total = None
        for step in steps_of(groups):
            taken = [arrivals[n][side] for n, side in step]
            blocks = [b for part, _ in taken for b in part]
            arrays = [columns] + [array for _, array in taken] + ([] if total is None else [total])
            (total,) = call(
                functools.partial(product_kernel, rows, blocks, len(step)),
                arrays,
                [((tokens.shape[0], width), F32)],
                flops=2 * tokens.shape[0] * len(blocks) * rows * width,
            )
        return total, arrivals[-1]

    def finish(parts):
        if rows % 128:
            return parts
        plans = [[b for blocks, _ in taken for b in blocks] for _, taken in parts]
        arrays = [columns]
        for total, taken in parts:
            arrays += [total] + [array for _, array in taken]
        return call(
            functools.partial(finish_kernel, rows, plans),
            arrays,
            [((tokens.shape[0], width), BF16)] * len(parts),
            hold=False,
        )

    def stream(pseudo, master, moment, s):
        sums = SUMS[s] if depth == 4 else plain_sums(depth)
        gathers = GATHERS[s] if depth == 4 else plain_gathers(depth)
        weights, state = weigh(reduce(pseudo, sums), master, moment)
        return project(*gather(weights, gathers)), state

    product_k, state_k = stream(pseudo_keys, master_keys, moment_keys, "k")
    product_v, state_v = stream(pseudo_values, master_values, moment_values, "v")
    return (*finish([product_k, product_v]), *state_k, *state_v)


def solution(mesh):
    spec = P(("groups", "replica"), None)
    stacked = P(("groups", "replica"), None, None)
    in_specs = (spec, stacked, stacked, spec, spec, spec, spec, P("groups"))
    out_specs = (spec,) * 6

    return jax.shard_map(body, mesh=mesh, in_specs=in_specs, out_specs=out_specs, check_vma=False)
```
